32 devices in a mesh: groups: 2 (over x), freq: 8 (over z, y), mgrp: 2 (over core).
Axes of the slice: x: 2, y: 2, z: 4, core: 2. Of those that a mesh axis runs over, the one named last changes fastest.
Arguments:
- seeds: int32 [32, 1024], P('groups', 'mgrp'), parts along dimension 0, may hold values from 0 to 1073741823
- noise_amp: float32 [512, 512], P(('groups', 'freq')), parts along dimension 0, may hold values from 0.3 to 3
- singular_projection: bfloat16 [32, 256, 16, 512], P('groups', 'freq'), parts along dimension 0, may hold values from -0.25 to 0.25
- kl_vecs: bfloat16 [32, 1536, 4096], P(('groups', 'freq'), 'mgrp'), parts along dimension 0, may hold values from -0.09375 to 0.09375
- m_order: int32 [32], P('groups'), parts along dimension 0, may hold values from 0 to 15, each once
- mode_counts: int32 [32], P('groups'), parts along dimension 0, may hold values from 384 to 1536, as said below
Outputs:
- kl_coeffs: bfloat16 [32, 1536, 1024], P(('groups', 'freq'), None, 'mgrp'), parts along dimension 0
The draws below stay inside these ranges and needn't reach their ends.
There are 2 independent parts, one for each index of `groups`. The reference program is written for one: setup_inputs(seed, part) draws one part's arguments, and reference() takes and returns one part's arrays. A program takes and returns all parts, laid end to end along the dimension named above; each array names one. Nothing has to cross between parts.
Inputs may be any that keep to these rules, and one draw needn't show every extreme that they name: `m_order`: each m appears in exactly one slot. `mode_counts`: some m keeps all 1536 modes.
All inputs are finite; a program needn't handle non-finite values.
Results may differ from the reference program's by a relative error of at most 0.0058.
Values may be sent and summed in bfloat16 or wider, within the bound.
A program may use at most 192 MiB of HBM per device.

```python
import math
import jax
import jax.numpy as jnp
from jax import lax

NF = 256
SVD_MODES = 16
NB = 512
KL_MAX = 1536
REALS = 1024
SVD_LEN = 4096
MS = 16


def draw_mode_counts(key, part):
    counts = jax.random.randint(key, (MS,), KL_MAX // 4, KL_MAX + 1, dtype=jnp.int32)
    chosen = jax.random.randint(jax.random.fold_in(key, 7), (), 0, MS, dtype=jnp.int32)
    return jnp.where(jnp.arange(MS, dtype=jnp.int32) == chosen, KL_MAX, counts).astype(jnp.int32)


def set_ends(array, key, least, top_value):
    place = [jax.random.randint(jax.random.fold_in(key, axis), (), 0, length) for axis, length in enumerate(array.shape)]
    main_axis = array.shape.index(max(array.shape))
    beside = place[:main_axis] + [(place[main_axis] + 1) % array.shape[main_axis]] + place[main_axis + 1:]
    return array.at[tuple(place)].set(least).at[tuple(beside)].set(top_value)


def shard_levels(rng, shape, shards, least, top_value):
    def one(axis_at, shards_of):
        draws = jax.random.uniform(jax.random.fold_in(jax.random.fold_in(rng, 6), axis_at), (shards_of,), jnp.float32, least / len(shards), top_value / len(shards))
        return jnp.repeat(jnp.exp(draws), shape[axis_at] // shards_of).reshape((-1,) + (1,) * (len(shape) - axis_at - 1))

    level = one(*shards[0])
    for cut in shards[1:]:
        level = level * one(*cut)
    return level


def normal_values(key, dims, scale, reach, shards=(), held_as=jnp.bfloat16):
    loudness = shard_levels(key, dims, shards, -0.22, 0.18) if shards else 1.0
    result = jax.random.normal(key, dims, jnp.float32) * scale * loudness
    return jnp.minimum(jnp.maximum(result, -reach), reach).astype(held_as)


def setup_inputs(seed: int = 0, part: int = 0) -> dict:
    key_list = jax.random.split(jax.random.key(seed), 7)
    own_keys = jax.random.split(jax.random.fold_in(key_list[6], part), 7)
    seeds = set_ends(jax.random.randint(own_keys[0], (MS, REALS), 0, 1073741824), jax.random.fold_in(own_keys[0], 1), 0, 1073741823).astype(jnp.int32)
    noise_amp = jnp.clip(jnp.exp(math.log(3.0) - 2.3025851 * jax.random.uniform(own_keys[1], (NF, NB), jnp.float32) ** shard_levels(own_keys[1], (NF, NB), ((0, 8),), -0.2, 0.2)), 0.3, 3.0)
    singular_projection = normal_values(own_keys[2], (MS, NF, SVD_MODES, NB), NB ** -0.5, 0.25, ((1, 8),))
    kl_vecs = normal_values(own_keys[3], (MS, KL_MAX, SVD_LEN), SVD_LEN ** -0.5, 0.09375, ((0, 8), (1, 2)))
    m_order = jax.random.permutation(own_keys[4], MS).astype(jnp.int32)
    mode_counts = draw_mode_counts(jax.random.fold_in(jax.random.fold_in(key_list[6], part), 71), part)
    return {"seeds": seeds, "noise_amp": noise_amp, "singular_projection": singular_projection, "kl_vecs": kl_vecs, "m_order": m_order, "mode_counts": mode_counts}


golden = 1640531527


def scramble(hashed_seed):
    hashed_seed = hashed_seed ^ ((hashed_seed >> 16) & 65535)
    hashed_seed = hashed_seed * 2146121005
    hashed_seed = hashed_seed ^ ((hashed_seed >> 15) & 131071)
    hashed_seed = hashed_seed * 1863026059
    hashed_seed = hashed_seed ^ ((hashed_seed >> 16) & 65535)
    return ((hashed_seed & 65535).astype(jnp.float32) - 32767.5) / 18918.0


def reference(seeds, noise_amp, singular_projection, kl_vecs, m_order, mode_counts):
    channel_index = jnp.arange(NF * NB, dtype=jnp.int32).reshape(NF, NB)
    mode_row_block = jnp.arange(KL_MAX, dtype=jnp.int32)

    def project(m_number):
        noise_draw = scramble(seeds[m_number][None, None, :] + channel_index[:, :, None] * golden)
        visible = (noise_amp[:, :, None] * noise_draw).astype(jnp.bfloat16)
        stacked = jnp.einsum("fkb,fbr->fkr", singular_projection[m_number].astype(jnp.float32), visible.astype(jnp.float32), precision=lax.Precision.HIGHEST)
        return stacked.astype(jnp.bfloat16).reshape(NF * SVD_MODES, REALS)

    def one_slot(position_index):
        m_number = m_order[position_index]
        vectors = project(m_number)
        coeffs = jnp.dot(kl_vecs[position_index], vectors, preferred_element_type=jnp.float32)
        kept_rows = mode_row_block[:, None] < mode_counts[m_number]
        return jnp.where(kept_rows, coeffs, jnp.float32(0.0)).astype(jnp.bfloat16)

    return lax.map(one_slot, jnp.arange(MS, dtype=jnp.int32))
```

```python
import functools

import jax
import jax.numpy as jnp
from jax import lax
from jax.experimental import pallas as pl
from jax.experimental.pallas import tpu as pltpu
from jax.sharding import PartitionSpec as P

golden = 1640531527


def wrapped(value):
    return (value + 2**31) % 2**32 - 2**31


def draw_kernel(base_ref, seeds_ref, weights_ref, out_ref, *, rows, depth, unroll):
    channels, modes, entries = weights_ref.shape[1:]
    reals = seeds_ref.shape[2]
    start = jnp.broadcast_to(seeds_ref[0], (rows, reals))
    start = start + lax.broadcasted_iota(jnp.int32, (rows, reals), 0) * golden
    base = base_ref[0]

    def scramble(shift):
        x = start + shift
        x = x ^ lax.shift_right_logical(x, 16)
        x = x * 2146121005
        x = x ^ lax.shift_right_logical(x, 15)
        x = x * 1863026059
        x = x ^ lax.shift_right_logical(x, 16)
        return ((x & 65535).astype(jnp.float32) - 32767.5).astype(jnp.bfloat16)

    def project(channel):
        first = base + channel * wrapped(entries * golden)
        total = None
        for top in range(0, entries, depth):
            drawn = jnp.concatenate(
                [scramble(first + wrapped(row * golden)) for row in range(top, top + depth, rows)], 0
            )
            part = jnp.dot(
                weights_ref[0, channel, :, top:top + depth], drawn, preferred_element_type=jnp.float32
            )
            total = part if total is None else total + part
        where = pl.ds(pl.multiple_of(channel * modes, modes), modes)
        out_ref[0, where, :] = total.astype(out_ref.dtype)

    def step(index, carry):
        for part in range(unroll):
            project(index * unroll + part)
        return carry

    lax.fori_loop(0, channels // unroll, step, 0)


def draw_and_project(base, seeds, weights):
    slots, channels, modes, entries = weights.shape
    reals = seeds.shape[2]
    unroll = 8 if channels % 8 == 0 else 1
    body = functools.partial(draw_kernel, rows=16, depth=min(256, entries), unroll=unroll)
    return pl.pallas_call(
        body,
        grid_spec=pltpu.PrefetchScalarGridSpec(
            num_scalar_prefetch=1,
            grid=(slots,),
            in_specs=[
                pl.BlockSpec((1, 1, reals), lambda s, b: (s, 0, 0)),
                pl.BlockSpec((1, channels, modes, entries), lambda s, b: (s, 0, 0, 0)),
            ],
            out_specs=pl.BlockSpec((1, channels * modes, reals), lambda s, b: (s, 0, 0)),
        ),
        out_shape=jax.ShapeDtypeStruct((slots, channels * modes, reals), jnp.bfloat16),
        cost_estimate=pl.CostEstimate(
            flops=slots * channels * entries * reals * 1500, bytes_accessed=0, transcendentals=0
        ),
        name="draw",
    )(base, seeds, weights)


def kl_kernel(scalars_ref, own_ref, other_ref, *refs):
    *vector_refs, out_ref = refs
    sources = len(vector_refs)
    slot, tile = pl.program_id(0), pl.program_id(1)
    core = scalars_ref[0]
    limit = scalars_ref[1 + sources + slot]
    tile_rows = own_ref.shape[1]
    half_rows = tile_rows * pl.num_programs(1)
    width = vector_refs[0].shape[1]
    for half, rows_ref in ((core, own_ref), (1 - core, other_ref)):
        total = None
        for number, vector_ref in enumerate(vector_refs):
            first = pl.multiple_of(scalars_ref[1 + number] * width, width)
            part = jnp.dot(
                rows_ref[0, :, pl.ds(first, width)], vector_ref[0], preferred_element_type=jnp.float32
            )
            total = part if total is None else total + part
        row = half * half_rows + tile * tile_rows + lax.broadcasted_iota(jnp.int32, total.shape, 0)
        out_ref[0, half] = jnp.where(row < limit, total, 0.0).astype(out_ref.dtype)


def kl_project(scalars, own, other, vectors):
    slots, half_rows, length = own.shape
    width, reals = vectors[0].shape[1:]
    tiles = 4
    tile_rows = half_rows // tiles
    rows_spec = pl.BlockSpec((1, tile_rows, length), lambda s, t, c: (s, t, 0))
    out = pl.pallas_call(
        kl_kernel,
        grid_spec=pltpu.PrefetchScalarGridSpec(
            num_scalar_prefetch=1,
            grid=(slots, tiles),
            in_specs=[rows_spec, rows_spec]
            + [pl.BlockSpec((1, width, reals), lambda s, t, c: (s, 0, 0))] * len(vectors),
            out_specs=pl.BlockSpec((1, 2, tile_rows, reals), lambda s, t, c: (s, 0, t, 0)),
        ),
        out_shape=jax.ShapeDtypeStruct((slots, 2, half_rows, reals), jnp.bfloat16),
        compiler_params=pltpu.CompilerParams(vmem_limit_bytes=48 * 1024 * 1024),
        cost_estimate=pl.CostEstimate(
            flops=4 * slots * half_rows * length * reals, bytes_accessed=4 * own.size, transcendentals=0
        ),
        name="kl",
    )(scalars, own, other, *vectors)
    return out.reshape(slots, 2 * half_rows, reals)


def hops(count):
    if count % 2:
        return [(shift, 0) for shift in range(1, count)], 1
    half = count // 2
    pairs = [(far, flip) for far in range(half) for flip in range(2) if far or flip]
    return sorted(pairs, key=lambda p: (min(p[0], half - p[0]) + p[1], p)), 2


def partner(index, far, flip, inner, count):
    outer = count // inner
    return (index // inner + far) % outer * inner + (index % inner + flip) % inner


def per_device(seeds, noise_amp, singular_projection, kl_vecs, m_order, mode_counts):
    count = lax.axis_size("freq")
    index = lax.axis_index("freq")
    channels, modes, entries = singular_projection.shape[1:]
    slots = kl_vecs.shape[0]
    cores = lax.axis_size("mgrp")
    scale = noise_amp[:, None, :] * (1.0 / 18918.0)

    def scaled_block(device):
        picked = []
        for slot in range(slots):
            m_number = lax.dynamic_index_in_dim(m_order, device * slots + slot, 0, keepdims=False)
            picked.append(lax.dynamic_index_in_dim(singular_projection, m_number, 0, keepdims=False))
        picked = jnp.stack(picked, 0).astype(jnp.float32)
        return (picked * scale[None]).astype(jnp.bfloat16)

    own_m = lax.dynamic_slice_in_dim(m_order, index * slots, slots, 0)
    own_seeds = jnp.take(seeds, own_m, axis=0, mode="clip")[:, None, :]
    limits = jnp.take(mode_counts, own_m, axis=0, mode="clip")

    order, inner = hops(count)
    blocks, sources = [scaled_block(index)], [index]
    for far, flip in order:
        outgoing = scaled_block(partner(index, far, flip, inner, count))
        links = [(d, partner(d, far, flip, inner, count)) for d in range(count)]
        blocks.append(lax.ppermute(outgoing, "freq", links))
        sources.append(partner(index, -far, -flip, inner, count))
    other_rows = lax.ppermute(kl_vecs, "mgrp", [(c, cores - 1 - c) for c in range(cores)])

    vectors = []
    for block, source in zip(blocks, sources):
        base = (source * (channels * entries) * golden).astype(jnp.int32)[None]
        vectors.append(draw_and_project(base, own_seeds, block))

    scalars = jnp.concatenate(
        [lax.axis_index("mgrp")[None], jnp.stack(sources), limits]
    ).astype(jnp.int32)
    return kl_project(scalars, kl_vecs, other_rows, vectors)


def solution(mesh):
    placed = (
        P("groups", "mgrp"),
        P(("groups", "freq"), None),
        P("groups", "freq", None, None),
        P(("groups", "freq"), "mgrp", None),
        P("groups"),
        P("groups"),
    )
    return jax.shard_map(
        per_device,
        mesh=mesh,
        in_specs=placed,
        out_specs=P(("groups", "freq"), None, "mgrp"),
        check_vma=False,
    )
```

```python
import functools

import jax
import jax.numpy as jnp
from jax import lax
from jax.experimental import pallas as pl
from jax.experimental.pallas import tpu as pltpu
from jax.sharding import PartitionSpec as P

golden = 1640531527
chunk = 8
vmem = 56 * 1024 * 1024


def wrapped(value):
    return (value + 2**31) % 2**32 - 2**31


def hops(count):
    if count % 2:
        return [(shift, 0) for shift in range(1, count)], 1
    half = count // 2
    pairs = [(far, flip) for far in range(half) for flip in range(2) if far or flip]
    return sorted(pairs, key=lambda p: (min(p[0], half - p[0]) + p[1], p)), 2


def partner(index, hop, inner, count):
    outer = count // inner
    far = lax.rem(lax.div(index, inner) + hop[0] % outer, outer)
    return far * inner + lax.rem(lax.rem(index, inner) + hop[1], inner)


def chosen(values, number):
    result = values[-1]
    for at in range(len(values) - 2, -1, -1):
        result = jnp.where(number == at, values[at], result)
    return result


def turn(number, block, slot, last_slot):
    return jnp.where(block == number, slot, jnp.where(block < number, 0, last_slot))


def scaled(block, amp_row):
    return (block.astype(jnp.float32) * (amp_row * (1.0 / 18918.0))).astype(jnp.bfloat16)


def scale_kernel(info_ref, order_ref, projection_ref, amp_ref, *refs, number):
    out_refs = refs[-number:]
    block = pl.program_id(0)
    channels = projection_ref.shape[1]
    for at, out_ref in enumerate(out_refs):
        @pl.when(block == at)
        def _():
            def step(channel, carry):
                out_ref[0, channel] = scaled(projection_ref[0, channel], amp_ref[pl.ds(channel, 1), :])
                return carry
            lax.fori_loop(0, channels, step, 0)


def scale_blocks(info, m_order, projection, amp, after, some_hops, inner, count, slots):
    channels, modes, entries = projection.shape[1:]
    number = len(some_hops)

    def picked(b, s, info_ref, order_ref):
        device = chosen([partner(info_ref[0], hop, inner, count) for hop in some_hops], b)
        return order_ref[device * slots + s], 0, 0, 0

    def placed(at):
        return lambda b, s, i, o: (turn(at, b, s, slots - 1), 0, 0, 0)

    shape = (1, channels, modes, entries)
    return pl.pallas_call(
        functools.partial(scale_kernel, number=number),
        grid_spec=pltpu.PrefetchScalarGridSpec(
            num_scalar_prefetch=2,
            grid=(number, slots),
            in_specs=[
                pl.BlockSpec(shape, picked),
                pl.BlockSpec((channels, entries), lambda b, s, i, o: (0, 0)),
            ] + [pl.BlockSpec(memory_space=pl.ANY)] * len(after),
            out_specs=[pl.BlockSpec(shape, placed(at)) for at in range(number)],
        ),
        out_shape=[jax.ShapeDtypeStruct((slots,) + shape[1:], jnp.bfloat16)] * number,
        compiler_params=pltpu.CompilerParams(vmem_limit_bytes=vmem),
        cost_estimate=pl.CostEstimate(flops=0, bytes_accessed=6_000_000, transcendentals=0),
        name="scale",
    )(info, m_order, projection, amp, *after)


def draw_chunk(seed_row, base, weights_ref, store, beside):
    channels, modes, entries = weights_ref.shape
    reals = seed_row.shape[1]
    rows, depth = 16, min(256, entries)
    start = jnp.broadcast_to(seed_row, (rows, reals))
    start = start + lax.broadcasted_iota(jnp.int32, (rows, reals), 0) * golden

    def scramble(shift):
        x = start + shift
        x = x ^ lax.shift_right_logical(x, 16)
        x = x * 2146121005
        x = x ^ lax.shift_right_logical(x, 15)
        x = x * 1863026059
        x = x ^ lax.shift_right_logical(x, 16)
        return ((x & 65535).astype(jnp.float32) - 32767.5).astype(jnp.bfloat16)

    for channel in range(channels):
        total = None
        for top in range(0, entries, depth):
            drawn = jnp.concatenate(
                [
                    scramble(base + wrapped((channel * entries + row) * golden))
                    for row in range(top, top + depth, rows)
                ],
                0,
            )
            part = jnp.dot(
                weights_ref[channel, :, top:top + depth], drawn, preferred_element_type=jnp.float32
            )
            total = part if total is None else total + part
        store(channel, total.astype(jnp.bfloat16))
        beside(channel)


def nothing(channel):
    pass


def base_of(source, piece, channels, entries):
    return (source * channels + piece * chunk) * wrapped(entries * golden)


def draw_own_kernel(info_ref, order_ref, seeds_ref, projection_ref, amp_ref, out_ref, held_ref, *, slots, channels):
    slot, piece = pl.program_id(0), pl.program_id(1)
    modes, entries = projection_ref.shape[2:]
    for channel in range(chunk):
        held_ref[channel] = scaled(projection_ref[0, channel], amp_ref[channel:channel + 1, :])
    m_number = order_ref[info_ref[0] * slots + slot]

    def store(channel, value):
        out_ref[0, channel * modes:(channel + 1) * modes, :] = value

    base = base_of(info_ref[0], piece, channels, entries)
    draw_chunk(seeds_ref[pl.ds(m_number, 1), :], base, held_ref, store, nothing)


def draw_own(info, m_order, seeds, projection, amp, slots):
    channels, modes, entries = projection.shape[1:]
    reals = seeds.shape[1]
    pieces = channels // chunk
    return pl.pallas_call(
        functools.partial(draw_own_kernel, slots=slots, channels=channels),
        grid_spec=pltpu.PrefetchScalarGridSpec(
            num_scalar_prefetch=2,
            grid=(slots, pieces),
            in_specs=[
                pl.BlockSpec(seeds.shape, lambda s, p, i, o: (0, 0)),
                pl.BlockSpec(
                    (1, chunk, modes, entries), lambda s, p, i, o: (o[i[0] * slots + s], p, 0, 0)
                ),
                pl.BlockSpec((chunk, entries), lambda s, p, i, o: (p, 0)),
            ],
            out_specs=pl.BlockSpec((1, chunk * modes, reals), lambda s, p, i, o: (s, p, 0)),
            scratch_shapes=[pltpu.VMEM((chunk, modes, entries), jnp.bfloat16)],
        ),
        out_shape=jax.ShapeDtypeStruct((slots, channels * modes, reals), jnp.bfloat16),
        cost_estimate=pl.CostEstimate(
            flops=slots * channels * entries * reals * 1500, bytes_accessed=0, transcendentals=0
        ),
        name="draw_own",
    )(info, m_order, seeds, projection, amp)


def draw_kernel(info_ref, order_ref, seeds_ref, *refs, slots, channels, some_hops, inner, count):
    number = len(some_hops)
    block_refs, out_ref, held_ref = refs[:number], refs[number], refs[number + 1]
    block, slot, piece = pl.program_id(0), pl.program_id(1), pl.program_id(2)
    modes, entries = held_ref.shape[1:]
    for at, block_ref in enumerate(block_refs):
        @pl.when(block == at)
        def _():
            held_ref[...] = block_ref[0]
    index = info_ref[0]
    source = chosen([partner(index, (-hop[0], hop[1]), inner, count) for hop in some_hops], block)
    m_number = order_ref[index * slots + slot]

    def store(channel, value):
        out_ref[0, 0, channel * modes:(channel + 1) * modes, :] = value

    base = base_of(source, piece, channels, entries)
    draw_chunk(seeds_ref[pl.ds(m_number, 1), :], base, held_ref, store, nothing)


def draw_blocks(info, m_order, seeds, blocks, some_hops, inner, count):
    slots, channels, modes, entries = blocks[0].shape
    reals = seeds.shape[1]
    pieces = channels // chunk
    number = len(blocks)

    def placed(at):
        return lambda b, s, p, i, o: (
            turn(at, b, s, slots - 1), turn(at, b, p, pieces - 1), 0, 0
        )

    return pl.pallas_call(
        functools.partial(
            draw_kernel, slots=slots, channels=channels, some_hops=some_hops, inner=inner, count=count
        ),
        grid_spec=pltpu.PrefetchScalarGridSpec(
            num_scalar_prefetch=2,
            grid=(number, slots, pieces),
            in_specs=[pl.BlockSpec(seeds.shape, lambda b, s, p, i, o: (0, 0))]
            + [pl.BlockSpec((1, chunk, modes, entries), placed(at)) for at in range(number)],
            out_specs=pl.BlockSpec(
                (1, 1, chunk * modes, reals), lambda b, s, p, i, o: (b, s, p, 0)
            ),
            scratch_shapes=[pltpu.VMEM((chunk, modes, entries), jnp.bfloat16)],
        ),
        out_shape=jax.ShapeDtypeStruct((number, slots, channels * modes, reals), jnp.bfloat16),
        cost_estimate=pl.CostEstimate(
            flops=number * slots * channels * entries * reals * 1500, bytes_accessed=0, transcendentals=0
        ),
        name="draw",
    )(info, m_order, seeds, *blocks)


def last_kernel(
    info_ref, order_ref, counts_ref, seeds_ref, block_ref, own_ref, other_ref, own_last_ref, other_last_ref,
    *refs, slots, channels, the_hops, groups, inner, count,
):
    group_refs = refs[:len(groups)]
    out_ref, vector_ref, total_ref = refs[len(groups):]
    slot, piece = pl.program_id(0), pl.program_id(1)
    pieces = channels // chunk
    modes, entries = block_ref.shape[2:]
    width = channels * modes
    tile_rows = own_ref.shape[1]
    half_rows = tile_rows * pieces
    index, core = info_ref[0], info_ref[1]
    m_number = order_ref[index * slots + slot]

    terms = []
    for group_ref, members in zip(group_refs, groups):
        for at, member in enumerate(members):
            source = index if member is None else partner(index, (-member[0], member[1]), inner, count)
            terms.append((source, group_ref, at))
    per_channel = [terms[at::chunk] for at in range(chunk)]

    def store(channel, value):
        first = pl.multiple_of(piece * (chunk * modes) + channel * modes, modes)
        vector_ref[pl.ds(first, modes), :] = value

    def beside(channel):
        for number, (source, group_ref, at) in enumerate(per_channel[channel]):
            first = pl.multiple_of(source * width, width)
            vectors = group_ref[at, 0]
            for half, rows_ref in enumerate((own_ref, other_ref)):
                part = jnp.dot(
                    rows_ref[0, :, pl.ds(first, width)], vectors, preferred_element_type=jnp.float32
                )
                if channel == 0 and number == 0:
                    total_ref[piece, half] = part
                else:
                    total_ref[piece, half] += part

    source = partner(index, (-the_hops[-1][0], the_hops[-1][1]), inner, count)
    base = base_of(source, piece, channels, entries)
    draw_chunk(seeds_ref[pl.ds(m_number, 1), :], base, block_ref.at[0], store, beside)

    @pl.when(piece == pieces - 1)
    def _():
        limit = counts_ref[m_number]

        def finish(tile, carry):
            for half, rows_ref in enumerate((own_last_ref, other_last_ref)):
                top = pl.multiple_of(tile * tile_rows, tile_rows)
                coeffs = total_ref[tile, half] + jnp.dot(
                    rows_ref[0, pl.ds(top, tile_rows), :], vector_ref[...], preferred_element_type=jnp.float32
                )
                place = core if half == 0 else 1 - core
                row = place * half_rows + top + lax.broadcasted_iota(jnp.int32, coeffs.shape, 0)
                out_ref[0, place, pl.ds(top, tile_rows), :] = jnp.where(
                    row < limit, coeffs, 0.0
                ).astype(out_ref.dtype)
            return carry

        lax.fori_loop(0, pieces, finish, 0)


def draw_last(info, m_order, mode_counts, seeds, block, own, other, group_vectors, the_hops, groups, inner, count):
    slots, channels, modes, entries = block.shape
    half_rows, length = own.shape[1:]
    reals = seeds.shape[1]
    pieces = channels // chunk
    width = channels * modes
    tile_rows = half_rows // pieces
    last = the_hops[-1]

    def last_columns(s, p, i, o, c):
        return s, 0, partner(i[0], (-last[0], last[1]), inner, count)

    rows_spec = pl.BlockSpec((1, tile_rows, length), lambda s, p, i, o, c: (s, p, 0))
    columns_spec = pl.BlockSpec((1, half_rows, width), last_columns)
    out = pl.pallas_call(
        functools.partial(
            last_kernel, slots=slots, channels=channels, the_hops=the_hops, groups=groups, inner=inner, count=count
        ),
        grid_spec=pltpu.PrefetchScalarGridSpec(
            num_scalar_prefetch=3,
            grid=(slots, pieces),
            in_specs=[
                pl.BlockSpec(seeds.shape, lambda s, p, i, o, c: (0, 0)),
                pl.BlockSpec((1, chunk, modes, entries), lambda s, p, i, o, c: (s, p, 0, 0)),
                rows_spec, rows_spec, columns_spec, columns_spec,
            ]
            + [
                pl.BlockSpec((v.shape[0], 1, width, reals), lambda s, p, i, o, c: (0, s, 0, 0))
                for v in group_vectors
            ],
            out_specs=pl.BlockSpec((1, 2, half_rows, reals), lambda s, p, i, o, c: (s, 0, 0, 0)),
            scratch_shapes=[
                pltpu.VMEM((width, reals), jnp.bfloat16),
                pltpu.VMEM((pieces, 2, tile_rows, reals), jnp.float32),
            ],
        ),
        out_shape=jax.ShapeDtypeStruct((slots, 2, half_rows, reals), jnp.bfloat16),
        compiler_params=pltpu.CompilerParams(vmem_limit_bytes=vmem),
        cost_estimate=pl.CostEstimate(
            flops=slots * channels * entries * reals * 1500, bytes_accessed=0, transcendentals=0
        ),
        name="draw_last",
    )(info, m_order, mode_counts, seeds, block, own, other, own, other, *group_vectors)
    return out.reshape(slots, 2 * half_rows, reals)


def per_device(seeds, noise_amp, singular_projection, kl_vecs, m_order, mode_counts):
    count = lax.axis_size("freq")
    cores = lax.axis_size("mgrp")
    slots = kl_vecs.shape[0]
    info = jnp.stack([lax.axis_index("freq"), lax.axis_index("mgrp")]).astype(jnp.int32)
    order, inner = hops(count)
    near, far = order[:3], order[3:]

    def send(blocks, some_hops):
        arrived = []
        for block, hop in zip(blocks, some_hops):
            links = [(d, to_device(d, hop, inner, count)) for d in range(count)]
            arrived.append(lax.ppermute(block, "freq", links))
        return arrived

    near_blocks = send(
        scale_blocks(info, m_order, singular_projection, noise_amp, (), near, inner, count, slots), near
    )
    own_vectors = draw_own(info, m_order, seeds, singular_projection, noise_amp, slots)
    far_blocks = send(
        scale_blocks(
            info, m_order, singular_projection, noise_amp, (own_vectors,), far, inner, count, slots
        ),
        far,
    )
    rows, _ = lax.optimization_barrier((kl_vecs, own_vectors))
    other_rows = lax.ppermute(rows, "mgrp", [(c, cores - 1 - c) for c in range(cores)])
    near_vectors = draw_blocks(info, m_order, seeds, near_blocks, near, inner, count)
    far_vectors = draw_blocks(info, m_order, seeds, far_blocks[:-1], far[:-1], inner, count)
    return draw_last(
        info, m_order, mode_counts, seeds, far_blocks[-1], kl_vecs, other_rows,
        [own_vectors[None], near_vectors, far_vectors], order, [[None], near, far[:-1]], inner, count,
    )


def to_device(device, hop, inner, count):
    outer = count // inner
    return (device // inner + hop[0]) % outer * inner + (device % inner + hop[1]) % inner


def solution(mesh):
    placed = (
        P("groups", "mgrp"),
        P(("groups", "freq"), None),
        P("groups", "freq", None, None),
        P(("groups", "freq"), "mgrp", None),
        P("groups"),
        P("groups"),
    )
    return jax.shard_map(
        per_device,
        mesh=mesh,
        in_specs=placed,
        out_specs=P(("groups", "freq"), None, "mgrp"),
        check_vma=False,
    )
```

```python
import functools

import jax
import jax.numpy as jnp
from jax import lax
from jax.experimental import pallas as pl
from jax.experimental.pallas import tpu as pltpu
from jax.sharding import PartitionSpec as P

golden = 1640531527
chunk = 8
vmem = 56 * 1024 * 1024


def wrapped(value):
    return (value + 2**31) % 2**32 - 2**31


def hops(count):
    if count % 2:
        return [(shift, 0) for shift in range(1, count)], 1
    half = count // 2
    pairs = [(far, flip) for far in range(half) for flip in range(2) if far or flip]
    return sorted(pairs, key=lambda p: (min(p[0], half - p[0]) + p[1], p)), 2


def partner(index, hop, inner, count):
    outer = count // inner
    far = lax.rem(lax.div(index, inner) + hop[0] % outer, outer)
    return far * inner + lax.rem(lax.rem(index, inner) + hop[1], inner)


def chosen(values, number):
    result = values[-1]
    for at in range(len(values) - 2, -1, -1):
        result = jnp.where(number == at, values[at], result)
    return result


def turn(number, block, slot, last_slot):
    return jnp.where(block == number, slot, jnp.where(block < number, 0, last_slot))


def scaled(block, amp_row):
    return (block.astype(jnp.float32) * (amp_row * (1.0 / 18918.0))).astype(jnp.bfloat16)


def scale_kernel(info_ref, order_ref, projection_ref, amp_ref, *refs, number):
    out_refs = refs[-number:]
    block = pl.program_id(0)
    channels = projection_ref.shape[1]
    for at, out_ref in enumerate(out_refs):
        @pl.when(block == at)
        def _():
            def step(group, carry):
                for part in range(chunk):
                    channel = group * chunk + part
                    out_ref[0, channel] = scaled(projection_ref[0, channel], amp_ref[pl.ds(channel, 1), :])
                return carry
            lax.fori_loop(0, channels // chunk, step, 0)


def scale_blocks(info, m_order, projection, amp, some_hops, inner, count, slots, parts):
    channels, modes, entries = projection.shape[1:]
    channels = channels // parts
    number = len(some_hops)

    def part_of(info_ref):
        return info_ref[1] if parts > 1 else 0

    def picked(b, s, info_ref, order_ref):
        device = chosen([partner(info_ref[0], hop, inner, count) for hop in some_hops], b)
        return order_ref[device * slots + s], part_of(info_ref), 0, 0

    def placed(at):
        return lambda b, s, i, o: (turn(at, b, s, slots - 1), 0, 0, 0)

    shape = (1, channels, modes, entries)
    return pl.pallas_call(
        functools.partial(scale_kernel, number=number),
        grid_spec=pltpu.PrefetchScalarGridSpec(
            num_scalar_prefetch=2,
            grid=(number, slots),
            in_specs=[
                pl.BlockSpec(shape, picked),
                pl.BlockSpec((channels, entries), lambda b, s, i, o: (part_of(i), 0)),
            ],
            out_specs=[pl.BlockSpec(shape, placed(at)) for at in range(number)],
        ),
        out_shape=[jax.ShapeDtypeStruct((slots,) + shape[1:], jnp.bfloat16)] * number,
        compiler_params=pltpu.CompilerParams(vmem_limit_bytes=vmem),
        cost_estimate=pl.CostEstimate(flops=0, bytes_accessed=6_000_000, transcendentals=0),
        name="scale",
    )(info, m_order, projection, amp)


def draw_chunk(seed_row, base, weights_ref, store, beside):
    channels, modes, entries = weights_ref.shape
    reals = seed_row.shape[1]
    rows, depth = 16, min(256, entries)
    start = jnp.broadcast_to(seed_row, (rows, reals))
    start = start + lax.broadcasted_iota(jnp.int32, (rows, reals), 0) * golden

    def scramble(shift):
        x = start + shift
        x = x ^ lax.shift_right_logical(x, 16)
        x = x * 2146121005
        x = x ^ lax.shift_right_logical(x, 15)
        x = x * 1863026059
        x = x ^ lax.shift_right_logical(x, 16)
        return ((x & 65535).astype(jnp.float32) - 32767.5).astype(jnp.bfloat16)

    for channel in range(channels):
        total = None
        for top in range(0, entries, depth):
            drawn = jnp.concatenate(
                [
                    scramble(base + wrapped((channel * entries + row) * golden))
                    for row in range(top, top + depth, rows)
                ],
                0,
            )
            part = jnp.dot(
                weights_ref[channel, :, top:top + depth], drawn, preferred_element_type=jnp.float32
            )
            total = part if total is None else total + part
        store(channel, total.astype(jnp.bfloat16))
        beside(channel)


def nothing(channel):
    pass


def base_of(source, piece, channels, entries):
    return (source * channels + piece * chunk) * wrapped(entries * golden)


def draw_own_kernel(info_ref, order_ref, seeds_ref, projection_ref, amp_ref, out_ref, held_ref, *, slots, channels):
    slot, piece = pl.program_id(0), pl.program_id(1)
    modes, entries = projection_ref.shape[2:]
    for channel in range(chunk):
        held_ref[channel] = scaled(projection_ref[0, channel], amp_ref[channel:channel + 1, :])
    m_number = order_ref[info_ref[0] * slots + slot]

    def store(channel, value):
        out_ref[0, channel * modes:(channel + 1) * modes, :] = value

    base = base_of(info_ref[0], piece, channels, entries)
    draw_chunk(seeds_ref[pl.ds(m_number, 1), :], base, held_ref, store, nothing)


def draw_own(info, m_order, seeds, projection, amp, slots):
    channels, modes, entries = projection.shape[1:]
    reals = seeds.shape[1]
    pieces = channels // chunk
    return pl.pallas_call(
        functools.partial(draw_own_kernel, slots=slots, channels=channels),
        grid_spec=pltpu.PrefetchScalarGridSpec(
            num_scalar_prefetch=2,
            grid=(slots, pieces),
            in_specs=[
                pl.BlockSpec(seeds.shape, lambda s, p, i, o: (0, 0)),
                pl.BlockSpec(
                    (1, chunk, modes, entries), lambda s, p, i, o: (o[i[0] * slots + s], p, 0, 0)
                ),
                pl.BlockSpec((chunk, entries), lambda s, p, i, o: (p, 0)),
            ],
            out_specs=pl.BlockSpec((1, chunk * modes, reals), lambda s, p, i, o: (s, p, 0)),
            scratch_shapes=[pltpu.VMEM((chunk, modes, entries), jnp.bfloat16)],
        ),
        out_shape=jax.ShapeDtypeStruct((slots, channels * modes, reals), jnp.bfloat16),
        cost_estimate=pl.CostEstimate(
            flops=slots * channels * entries * reals * 1500, bytes_accessed=0, transcendentals=0
        ),
        name="draw_own",
    )(info, m_order, seeds, projection, amp)


def hold(held_ref, part_refs, wanted, piece, channels, core):
    each = channels // chunk // len(part_refs)
    for number, part_ref in enumerate(part_refs):
        here = wanted
        if len(part_refs) > 1:
            mine = lax.div(piece, each) == core
            here = here & (mine if number == 0 else ~mine)

        @pl.when(here)
        def _():
            held_ref[...] = part_ref[0]


def draw_kernel(info_ref, order_ref, seeds_ref, *refs, slots, channels, parts, some_hops, inner, count):
    number = len(some_hops)
    block_refs, out_ref, held_ref = refs[:number * parts], refs[number * parts], refs[number * parts + 1]
    block, slot, piece = pl.program_id(0), pl.program_id(1), pl.program_id(2)
    modes, entries = held_ref.shape[1:]
    for at in range(number):
        hold(held_ref, block_refs[at * parts:(at + 1) * parts], block == at, piece, channels, info_ref[1])
    index = info_ref[0]
    source = chosen([partner(index, (-hop[0], hop[1]), inner, count) for hop in some_hops], block)
    m_number = order_ref[index * slots + slot]

    def store(channel, value):
        out_ref[0, 0, channel * modes:(channel + 1) * modes, :] = value

    base = base_of(source, piece, channels, entries)
    draw_chunk(seeds_ref[pl.ds(m_number, 1), :], base, held_ref, store, nothing)


def draw_blocks(info, m_order, seeds, blocks, some_hops, inner, count):
    parts = len(blocks[0])
    slots, channels, modes, entries = blocks[0][0].shape
    each = channels // chunk
    channels = channels * parts
    reals = seeds.shape[1]
    pieces = channels // chunk
    number = len(blocks)

    def placed(at):
        return lambda b, s, p, i, o: (
            turn(at, b, s, slots - 1), turn(at, b, lax.rem(p, each), each - 1), 0, 0
        )

    return pl.pallas_call(
        functools.partial(
            draw_kernel, slots=slots, channels=channels, parts=parts, some_hops=some_hops, inner=inner, count=count
        ),
        grid_spec=pltpu.PrefetchScalarGridSpec(
            num_scalar_prefetch=2,
            grid=(number, slots, pieces),
            in_specs=[pl.BlockSpec(seeds.shape, lambda b, s, p, i, o: (0, 0))]
            + [pl.BlockSpec((1, chunk, modes, entries), placed(at)) for at in range(number) for _ in range(parts)],
            out_specs=pl.BlockSpec(
                (1, 1, chunk * modes, reals), lambda b, s, p, i, o: (b, s, p, 0)
            ),
            scratch_shapes=[pltpu.VMEM((chunk, modes, entries), jnp.bfloat16)],
        ),
        out_shape=jax.ShapeDtypeStruct((number, slots, channels * modes, reals), jnp.bfloat16),
        cost_estimate=pl.CostEstimate(
            flops=number * slots * channels * entries * reals * 1500, bytes_accessed=0, transcendentals=0
        ),
        name="draw",
    )(info, m_order, seeds, *[part for block in blocks for part in block])


def last_kernel(
    info_ref, order_ref, counts_ref, seeds_ref, own_ref, other_ref, own_last_ref, other_last_ref,
    *refs, slots, channels, parts, the_hops, groups, inner, count,
):
    group_refs, refs = refs[:len(groups)], refs[len(groups):]
    part_refs = refs[:parts]
    out_ref, vector_ref, total_ref, held_ref = refs[parts:]
    slot, piece = pl.program_id(0), pl.program_id(1)
    pieces = channels // chunk
    modes, entries = held_ref.shape[1:]
    hold(held_ref, part_refs, piece >= 0, piece, channels, info_ref[1])
    width = channels * modes
    tile_rows = own_ref.shape[1]
    half_rows = tile_rows * pieces
    index, core = info_ref[0], info_ref[1]
    m_number = order_ref[index * slots + slot]

    terms = []
    for group_ref, members in zip(group_refs, groups):
        for at, member in enumerate(members):
            source = index if member is None else partner(index, (-member[0], member[1]), inner, count)
            terms.append((source, group_ref, at))
    per_channel = [terms[at::chunk] for at in range(chunk)]

    def store(channel, value):
        first = pl.multiple_of(piece * (chunk * modes) + channel * modes, modes)
        vector_ref[pl.ds(first, modes), :] = value

    def beside(channel):
        for number, (source, group_ref, at) in enumerate(per_channel[channel]):
            first = pl.multiple_of(source * width, width)
            rows = jnp.concatenate([own_ref[0, :, pl.ds(first, width)], other_ref[0, :, pl.ds(first, width)]], 0)
            part = jnp.dot(rows, group_ref[at, 0], preferred_element_type=jnp.float32)
            if channel == 0 and number == 0:
                total_ref[piece] = part
            else:
                total_ref[piece] += part

    source = partner(index, (-the_hops[-1][0], the_hops[-1][1]), inner, count)
    base = base_of(source, piece, channels, entries)
    draw_chunk(seeds_ref[pl.ds(m_number, 1), :], base, held_ref, store, beside)

    @pl.when(piece == pieces - 1)
    def _():
        limit = counts_ref[m_number]

        def finish(tile, carry):
            for half, rows_ref in enumerate((own_last_ref, other_last_ref)):
                top = pl.multiple_of(tile * tile_rows, tile_rows)
                coeffs = total_ref[tile, half * tile_rows:(half + 1) * tile_rows] + jnp.dot(
                    rows_ref[0, pl.ds(top, tile_rows), :], vector_ref[...], preferred_element_type=jnp.float32
                )
                place = core if half == 0 else 1 - core
                row = place * half_rows + top + lax.broadcasted_iota(jnp.int32, coeffs.shape, 0)
                out_ref[0, place, pl.ds(top, tile_rows), :] = jnp.where(
                    row < limit, coeffs, 0.0
                ).astype(out_ref.dtype)
            return carry

        lax.fori_loop(0, pieces, finish, 0)


def draw_last(info, m_order, mode_counts, seeds, block, own, other, group_vectors, the_hops, groups, inner, count):
    parts = len(block)
    slots, channels, modes, entries = block[0].shape
    each = channels // chunk
    channels = channels * parts
    half_rows, length = own.shape[1:]
    reals = seeds.shape[1]
    pieces = channels // chunk
    width = channels * modes
    tile_rows = half_rows // pieces
    last = the_hops[-1]

    def last_columns(s, p, i, o, c):
        return s, 0, partner(i[0], (-last[0], last[1]), inner, count)

    rows_spec = pl.BlockSpec((1, tile_rows, length), lambda s, p, i, o, c: (s, p, 0))
    columns_spec = pl.BlockSpec((1, half_rows, width), last_columns)
    out = pl.pallas_call(
        functools.partial(
            last_kernel, slots=slots, channels=channels, parts=parts, the_hops=the_hops, groups=groups, inner=inner, count=count
        ),
        grid_spec=pltpu.PrefetchScalarGridSpec(
            num_scalar_prefetch=3,
            grid=(slots, pieces),
            in_specs=[
                pl.BlockSpec(seeds.shape, lambda s, p, i, o, c: (0, 0)),
                rows_spec, rows_spec, columns_spec, columns_spec,
            ]
            + [
                pl.BlockSpec((v.shape[0], 1, width, reals), lambda s, p, i, o, c: (0, s, 0, 0))
                for v in group_vectors
            ]
            + [
                pl.BlockSpec(
                    (1, chunk, modes, entries), lambda s, p, i, o, c: (s, lax.rem(p, each), 0, 0)
                )
            ] * parts,
            out_specs=pl.BlockSpec((1, 2, half_rows, reals), lambda s, p, i, o, c: (s, 0, 0, 0)),
            scratch_shapes=[
                pltpu.VMEM((width, reals), jnp.bfloat16),
                pltpu.VMEM((pieces, 2 * tile_rows, reals), jnp.float32),
                pltpu.VMEM((chunk, modes, entries), jnp.bfloat16),
            ],
        ),
        out_shape=jax.ShapeDtypeStruct((slots, 2, half_rows, reals), jnp.bfloat16),
        compiler_params=pltpu.CompilerParams(vmem_limit_bytes=vmem),
        cost_estimate=pl.CostEstimate(
            flops=slots * channels * entries * reals * 1500, bytes_accessed=0, transcendentals=0
        ),
        name="draw_last",
    )(info, m_order, mode_counts, seeds, own, other, own, other, *group_vectors, *block)
    return out.reshape(slots, 2 * half_rows, reals)


def per_device(seeds, noise_amp, singular_projection, kl_vecs, m_order, mode_counts):
    count = lax.axis_size("freq")
    cores = lax.axis_size("mgrp")
    slots = kl_vecs.shape[0]
    info = jnp.stack([lax.axis_index("freq"), lax.axis_index("mgrp")]).astype(jnp.int32)
    order, inner = hops(count)
    near, far = order[:3], order[3:]

    def send(blocks, some_hops):
        arrived = []
        for block, hop in zip(blocks, some_hops):
            links = [(d, to_device(d, hop, inner, count)) for d in range(count)]
            arrived.append(lax.ppermute(block, "freq", links))
        return arrived

    swap = [(c, cores - 1 - c) for c in range(cores)]
    shared = cores == 2 and singular_projection.shape[1] % (2 * chunk) == 0
    near_scaled = scale_blocks(info, m_order, singular_projection, noise_amp, near, inner, count, slots, 1)
    near_blocks = send(near_scaled, near)
    later_info, _ = lax.optimization_barrier((info, near_scaled))
    far_blocks = send(
        scale_blocks(
            later_info, m_order, singular_projection, noise_amp, far, inner, count, slots, 2 if shared else 1
        ),
        far,
    )
    own_vectors = draw_own(info, m_order, seeds, singular_projection, noise_amp, slots)
    rows, _ = lax.optimization_barrier((kl_vecs, own_vectors))
    other_rows = lax.ppermute(rows, "mgrp", swap)
    first_vectors = draw_blocks(info, m_order, seeds, [(b,) for b in near_blocks[:2]], near[:2], inner, count)
    if shared:
        far_blocks, _ = lax.optimization_barrier((far_blocks, first_vectors))
        far_blocks = [(block, lax.ppermute(block, "mgrp", swap)) for block in far_blocks]
    else:
        far_blocks = [(block,) for block in far_blocks]
    second_vectors = draw_blocks(info, m_order, seeds, [(b,) for b in near_blocks[2:]], near[2:], inner, count)
    far_vectors = draw_blocks(info, m_order, seeds, far_blocks[:-1], far[:-1], inner, count)
    return draw_last(
        info, m_order, mode_counts, seeds, far_blocks[-1], kl_vecs, other_rows,
        [own_vectors[None], first_vectors, second_vectors, far_vectors], order,
        [[None], near[:2], near[2:], far[:-1]], inner, count,
    )


def to_device(device, hop, inner, count):
    outer = count // inner
    return (device // inner + hop[0]) % outer * inner + (device % inner + hop[1]) % inner


def solution(mesh):
    placed = (
        P("groups", "mgrp"),
        P(("groups", "freq"), None),
        P("groups", "freq", None, None),
        P(("groups", "freq"), "mgrp", None),
        P("groups"),
        P("groups"),
    )
    return jax.shard_map(
        per_device,
        mesh=mesh,
        in_specs=placed,
        out_specs=P(("groups", "freq"), None, "mgrp"),
        check_vma=False,
    )
```
